32 devices in a mesh: dp: 8 (over y, x, core), tensor: 4 (over z).
Axes of the slice: x: 2, y: 2, z: 4, core: 2. Of those that a mesh axis runs over, the one named last changes fastest.
Arguments:
- activations: bfloat16 [3072, 16384], P(('dp', 'tensor')), may hold values from -6 to 6
- out_grad: bfloat16 [3072, 16384], P('dp', 'tensor'), may hold values from -0.25 to 0.25
- block_ids: int32 [4, 12], replicated, may hold values from 0 to 127, as said below
- owner_map: int32 [8, 4], replicated, may hold values from 0 to 1, as said below
- master: float32 [1024, 16384], P('dp', 'tensor'), may hold values from -3 to 3
- moment: float32 [1024, 16384], P('dp', 'tensor'), may hold values from -3 to 3
- second: float32 [1024, 16384], P('dp', 'tensor'), may hold values from 0.01 to 2
Outputs:
- new_master: float32 [1024, 16384], P('dp', 'tensor')
- new_moment: float32 [1024, 16384], P('dp', 'tensor')
- new_second: float32 [1024, 16384], P('dp', 'tensor')
- hot_weights: bfloat16 [1024, 16384], P('dp')
- cold_recv: float32 [4096, 16384], P('dp', 'tensor')
The draws below stay inside these ranges and needn't reach their ends.
Inputs may be any that keep to these rules, and one draw needn't show every extreme that they name: `block_ids`: the 12 block numbers in a row are distinct. `owner_map`: each row has between 1 and 3 ones; some row has exactly 3 ones and some row exactly 1.
All inputs are finite; a program needn't handle non-finite values.
Results may differ from the reference program's by a relative error of at most 0.006.
Values may be sent and summed in bfloat16 or wider, within the bound.
No kernel may reach another device: no remote copies, remote signals or barrier semaphores. Data moves between devices by JAX's collectives and lax.ppermute only.
A program may use at most 128 MiB of HBM per device.

```python
import math
import jax
import jax.numpy as jnp
from jax import lax

D = 16384
QO = 16384
BLOCK = 128
HOT = 8
COLD = 4
MOSTC = 3
TOK = 384
TOKENS = 3072
HOTR = 1024
N_DP = 8
N_TENSOR = 4


def draw_block_ids(key, part):
    keys = jax.random.split(jax.random.fold_in(key, 11), N_TENSOR)
    rows = jax.vmap(lambda single: jax.random.permutation(single, D // BLOCK)[:HOT + COLD])(keys)
    return rows.astype(jnp.int32)


def draw_owner_map(key, part):
    base = jax.random.fold_in(key, 23)
    first, second_key, third = jax.random.split(base, 3)
    counts = jax.random.randint(first, (N_DP,), COLD - MOSTC, MOSTC + 1)
    chosen = jax.random.permutation(second_key, N_DP)
    counts = counts.at[chosen[0]].set(MOSTC).at[chosen[1]].set(COLD - MOSTC)
    ranks = jax.vmap(lambda single: jax.random.permutation(single, COLD))(jax.random.split(third, N_DP))
    return (ranks < counts[:, None]).astype(jnp.int32)


def shard_levels(rng, shape, cuts, low, high):
    loudness, own = 1.0, jax.random.fold_in(rng, 6)
    for position, parts in cuts:
        draws = jnp.exp(jax.random.uniform(jax.random.fold_in(own, position), (parts,), jnp.float32, low / len(cuts), high / len(cuts)))
        loudness = loudness * jnp.repeat(draws, shape[position] // parts).reshape([-1 if axis == position else 1 for axis in range(len(shape))])
    return loudness


def bell_draw(own_key, extent, deviation, limit, shards=(), kind=jnp.bfloat16):
    factor_of = shard_levels(own_key, extent, shards, -0.22, 0.18) if shards else 1.0
    entries = jax.random.normal(own_key, extent, jnp.float32) * deviation * factor_of
    return jnp.minimum(jnp.maximum(entries, -limit), limit).astype(kind)


def setup_inputs(seed: int = 0) -> dict:
    streams_of = jax.random.split(jax.random.key(seed), 8)
    activations = bell_draw(streams_of[0], (TOKENS, D), 1.0, 6.0, ((0, 32),))
    out_grad = bell_draw(streams_of[1], (TOKENS, QO), (1.0 / TOKENS ** 0.5), 0.25, ((0, 8), (1, 4)))
    block_ids = draw_block_ids(jax.random.fold_in(streams_of[7], 71), 0)
    owner_map = draw_owner_map(jax.random.fold_in(streams_of[7], 71), 0)
    master = bell_draw(streams_of[4], (HOTR, QO), 0.5, 3.0, ((0, 8), (1, 4)), jnp.float32)
    moment = bell_draw(streams_of[5], (HOTR, QO), 0.5, 3.0, ((0, 8), (1, 4)), jnp.float32)
    second = jnp.clip(jnp.exp(math.log(2.0) - 5.2983174 * jax.random.uniform(streams_of[6], (HOTR, QO), jnp.float32) ** shard_levels(streams_of[6], (HOTR, QO), ((0, 8), (1, 4)), -0.2, 0.2)), 0.01, 2.0)
    return {"activations": activations, "out_grad": out_grad, "block_ids": block_ids, "owner_map": owner_map, "master": master, "moment": moment, "second": second}


BETA_ONE = 0.9
BETA_TWO = 0.95
ADAM_EPS = 1e-08
LEARN_RATE = 0.01
DECAY = 0.1
CORRECT_ONE = 1.0 - 0.9 ** 10
CORRECT_TWO = 1.0 - 0.95 ** 10

def pick_blocks(tok_rows, block_row):
    shaped = tok_rows.reshape(tok_rows.shape[0], D // BLOCK, BLOCK)
    return shaped[:, block_row, :].reshape(tok_rows.shape[0], block_row.shape[0] * BLOCK)

def reference(activations, out_grad, block_ids, owner_map, master, moment, second):
    qloc = QO // N_TENSOR
    hot_rows = HOT * BLOCK

    def per_index(carry, index):
        tok_rows = lax.dynamic_slice_in_dim(activations, index * TOK, TOK, 0)
        grad_rows = lax.dynamic_slice_in_dim(out_grad, index * TOK, TOK, 0)
        hot_list = []
        cold_list = []
        for group in range(N_TENSOR):
            chosen = pick_blocks(tok_rows, block_ids[group]).astype(jnp.float32)
            grad_cols = grad_rows[:, group * qloc:(group + 1) * qloc].astype(jnp.float32)
            product = jnp.dot(chosen.T, grad_cols, preferred_element_type=jnp.float32)
            hot_list.append(product[:hot_rows].astype(jnp.bfloat16).astype(jnp.float32))
            cold_list.append(product[hot_rows:].astype(jnp.bfloat16))
        return (carry + jnp.stack(hot_list), jnp.stack(cold_list))
    start_sum = jnp.zeros((N_TENSOR, hot_rows, qloc), jnp.float32)
    hot_sum, cold_parts = lax.scan(per_index, start_sum, jnp.arange(N_DP, dtype=jnp.int32))
    grad = hot_sum.transpose(1, 0, 2).reshape(hot_rows, QO)
    cold_parts = cold_parts.reshape(N_DP, N_TENSOR, COLD, BLOCK, qloc)
    from_prev = jnp.roll(cold_parts, 1, axis=0)
    from_next = jnp.roll(cold_parts, -1, axis=0)
    prev_owner = jnp.roll(owner_map, 1, axis=0)[:, None, :, None, None]
    next_owner = jnp.roll(owner_map, -1, axis=0)[:, None, :, None, None]
    total = jnp.where(prev_owner == 1, from_prev.astype(jnp.float32), 0.0)
    total = total + jnp.where(next_owner == 0, from_next.astype(jnp.float32), 0.0)
    cold_recv = total.transpose(0, 2, 3, 1, 4).reshape(N_DP * COLD * BLOCK, QO)
    new_moment = BETA_ONE * moment + (1.0 - BETA_ONE) * grad
    new_second = BETA_TWO * second + (1.0 - BETA_TWO) * grad * grad
    update = new_moment / CORRECT_ONE / (jnp.sqrt(new_second / CORRECT_TWO) + ADAM_EPS)
    new_master = master - LEARN_RATE * (update + DECAY * master)
    hot_weights = new_master.astype(jnp.bfloat16)
    return (new_master, new_moment, new_second, hot_weights, cold_recv)
```

```python
import jax
import jax.numpy as jnp
from jax import lax
from jax.experimental import pallas as pl
from jax.experimental.pallas import tpu as pltpu
from jax.sharding import PartitionSpec as P

BLOCK = 128
HOT = 8
COLD = 4
CHUNKS = 2

BETA_ONE = 0.9
BETA_TWO = 0.95
ADAM_EPS = 1e-08
LEARN_RATE = 0.01
DECAY = 0.1
CORRECT_ONE = 1.0 - 0.9**10
CORRECT_TWO = 1.0 - 0.95**10


f32 = jnp.float32
bf16 = jnp.bfloat16
ANY = pl.BlockSpec(memory_space=pl.ANY)
SMEM = pl.BlockSpec(memory_space=pltpu.SMEM)
CONTRACT = (((0,), (0,)), ((), ()))


def adam(master, moment, second, grad):
    new_moment = BETA_ONE * moment + (1.0 - BETA_ONE) * grad
    new_second = BETA_TWO * second + (1.0 - BETA_TWO) * grad * grad
    update = new_moment / CORRECT_ONE / (jnp.sqrt(new_second / CORRECT_TWO) + ADAM_EPS)
    new_master = master - LEARN_RATE * (update + DECAY * master)
    return new_master, new_moment, new_second


def gather_blocks(activations, table, groups):
    rows = activations.shape[0]
    total = sum(count for _, _, count in groups)

    def body(table_ref, src, *rest):
        outs, sems = rest[:-1], rest[-1]
        copies = []
        for out, (row, first, count) in zip(outs, groups):
            for slot in range(count):
                start = pl.multiple_of(table_ref[row, first + slot] * BLOCK, BLOCK)
                copies.append(
                    pltpu.make_async_copy(
                        src.at[:, pl.ds(start, BLOCK)],
                        out.at[:, pl.ds(slot * BLOCK, BLOCK)],
                        sems.at[len(copies)],
                    )
                )
                copies[-1].start()
        for copy in copies:
            copy.wait()

    return pl.pallas_call(
        body,
        in_specs=[SMEM, ANY],
        out_specs=[ANY] * len(groups),
        out_shape=[jax.ShapeDtypeStruct((rows, count * BLOCK), activations.dtype) for _, _, count in groups],
        scratch_shapes=[pltpu.SemaphoreType.DMA((total,))],
        name="gather_blocks",
    )(table, activations)


def product(place, piece_sets, rhs_list, first_col, ncols, tile, row_counts):
    nset = len(piece_sets)
    npiece = len(piece_sets[0])
    rows, width = piece_sets[0][0].shape
    depth = rows * npiece
    qlocal = rhs_list[0].shape[1]

    def body(place_ref, *rest):
        pieces = rest[: nset * npiece]
        rhs = rest[nset * npiece : nset * npiece + nset]
        outs = rest[nset * npiece + nset : -1]
        lhs = rest[-1]

        @pl.when(pl.program_id(0) == 0)
        def _():
            for s in range(nset):
                for k in range(npiece):
                    at = pl.multiple_of(s * depth + place_ref[k] * rows, rows)
                    lhs[pl.ds(at, rows), :] = pieces[s * npiece + k][...]

        row = 0
        for out, count in zip(outs, row_counts):
            acc = None
            for s in range(nset):
                part = lax.dot_general(
                    lhs[s * depth : (s + 1) * depth, row : row + count],
                    rhs[s][...],
                    CONTRACT,
                    preferred_element_type=f32,
                )
                acc = part if acc is None else acc + part
            out[...] = acc.astype(out.dtype)
            row += count

    base = first_col // tile
    return pl.pallas_call(
        body,
        grid=(ncols // tile,),
        in_specs=[SMEM]
        + [pl.BlockSpec((rows, width), lambda g: (0, 0))] * (nset * npiece)
        + [pl.BlockSpec((depth, tile), lambda g: (0, base + g))] * nset,
        out_specs=[pl.BlockSpec((count, tile), lambda g: (0, g)) for count in row_counts],
        out_shape=[jax.ShapeDtypeStruct((count, ncols), bf16) for count in row_counts],
        scratch_shapes=[pltpu.VMEM((nset * depth, width), bf16)],
        cost_estimate=pl.CostEstimate(
            flops=2 * nset * depth * width * ncols,
            bytes_accessed=2 * (nset * depth * (width + ncols) + width * ncols),
            transcendentals=0,
        ),
        name="product",
    )(place, *[p for ps in piece_sets for p in ps], *rhs_list)


def adam_chunk(state, done, parts, first_col, tile):
    rows, qlocal = state[0].shape
    ncols = parts[0][0].shape[1]
    npart = len(parts)
    base = first_col // tile

    def body(*refs):
        ins = refs[:3]
        addends = refs[3 : 3 + npart]
        outs = refs[-4:]
        grad = addends[0][...].astype(f32)
        for ref in addends[1:]:
            grad = grad + ref[...].astype(f32)
        new = adam(ins[0][...], ins[1][...], ins[2][...], grad)
        for out, value in zip(outs[:3], new):
            out[...] = value
        outs[3][...] = new[0].astype(bf16)

    wide = pl.BlockSpec((rows, tile), lambda g: (0, base + g))
    part_specs = [pl.BlockSpec((rows, tile), lambda g, r=first // rows: (r, g)) for _, first in parts]
    extra = [] if done is None else list(done)
    return pl.pallas_call(
        body,
        grid=(ncols // tile,),
        in_specs=[wide] * 3 + part_specs + [ANY] * len(extra),
        out_specs=[wide] * 3 + [pl.BlockSpec((rows, tile), lambda g: (0, g))],
        out_shape=[jax.ShapeDtypeStruct((rows, qlocal), f32)] * 3 + [jax.ShapeDtypeStruct((rows, ncols), bf16)],
        input_output_aliases={3 + npart + i: i for i in range(len(extra))},
        cost_estimate=pl.CostEstimate(flops=20 * rows * ncols, bytes_accessed=34 * rows * ncols, transcendentals=0),
        name="adam_chunk",
    )(*state, *[p for p, _ in parts], *extra)


def combine_cold(flags, prev_slots, next_slots, tile):
    slots = list(prev_slots) + list(next_slots)
    rows, qlocal = slots[0].shape

    def body(flags_ref, *refs):
        out = refs[-1]
        values = [ref[...].astype(f32) for ref in refs[:-1]]
        for c in range(COLD):
            acc = jnp.zeros((rows, tile), f32)
            for s, value in enumerate(values):
                acc = acc + jnp.where(flags_ref[c, s] == 1, value, 0.0)
            out[c * rows : (c + 1) * rows, :] = acc

    return pl.pallas_call(
        body,
        grid=(qlocal // tile,),
        in_specs=[SMEM] + [pl.BlockSpec((rows, tile), lambda g: (0, g))] * len(slots),
        out_specs=pl.BlockSpec((COLD * rows, tile), lambda g: (0, g)),
        out_shape=jax.ShapeDtypeStruct((COLD * rows, qlocal), f32),
        cost_estimate=pl.CostEstimate(flops=48 * rows * qlocal, bytes_accessed=28 * rows * qlocal, transcendentals=0),
        name="combine_cold",
    )(flags, *slots)


def fast_device(activations, out_grad, block_ids, owner_map, master, moment, second):
    n_dp = lax.axis_size("dp")
    n_t = lax.axis_size("tensor")
    dp = lax.axis_index("dp")
    t = lax.axis_index("tensor")
    qlocal = out_grad.shape[1]
    half = n_dp // 2

    def swap(block, mask):
        return lax.ppermute(block, "dp", [(i, i ^ mask) for i in range(n_dp)])

    grad_pair = swap(out_grad, 1)

    flip = [half | 2, half, 2, 0]
    hot_order = jnp.stack([dp ^ 1 ^ m for m in flip] + [dp ^ m for m in flip])
    ranks = jnp.where(
        owner_map == 1,
        jnp.cumsum(owner_map, axis=1) - owner_map,
        jnp.sum(owner_map, axis=1, keepdims=True) + jnp.cumsum(1 - owner_map, axis=1) - (1 - owner_map),
    )
    my_ranks = ranks[dp]
    slot_ids = jnp.arange(COLD, dtype=jnp.int32)
    cold_order = jnp.sum(jnp.where(my_ranks[None, :] == slot_ids[:, None], slot_ids[None, :], 0), axis=1)
    order = jnp.concatenate([hot_order.astype(jnp.int32), HOT + cold_order.astype(jnp.int32)])
    dest = (t + jnp.arange(n_t, dtype=jnp.int32)) % n_t
    table = block_ids[dest[:, None], order[None, :]]

    pair = HOT // 2
    groups = []
    for k in range(n_t):
        groups += [(k, 0, pair), (k, pair, pair), (k, HOT, COLD)]
    gathered = gather_blocks(activations, table, groups)

    def to_group(block, k):
        if k == 0:
            return block
        return lax.ppermute(block, "tensor", [(i, (i + k) % n_t) for i in range(n_t)])

    def to_group_pair(block, k):
        route = [(d * n_t + i, (d ^ 1) * n_t + (i + k) % n_t) for d in range(n_dp) for i in range(n_t)]
        return lax.ppermute(block, ("dp", "tensor"), route)

    mine, theirs, cold = [], [], []
    for k in range(n_t):
        theirs.append(to_group_pair(gathered[3 * k], k))
        mine.append(to_group(gathered[3 * k + 1], k))
    for k in range(n_t):
        cold.append(to_group(gathered[3 * k + 2], k))
    place = (t - jnp.arange(n_t, dtype=jnp.int32)) % n_t

    width = qlocal // CHUNKS
    tile = min(512, width)
    kept, arrived = [], []
    for q in range(CHUNKS):
        send, keep = product(place, [mine, theirs], [out_grad, grad_pair], q * width, width, tile, [2 * BLOCK, 2 * BLOCK])
        kept.append(keep)
        arrived.append(swap(send, half))

    slots = product(place, [cold], [out_grad], 0, qlocal, tile, [BLOCK] * COLD)
    ahead = [(i, (i + 1) % n_dp) for i in range(n_dp)]
    back = [(i, (i - 1) % n_dp) for i in range(n_dp)]

    done = None
    hot = []
    for q in range(CHUNKS):
        forward = (arrived[q][:BLOCK].astype(f32) + kept[q][:BLOCK].astype(f32)).astype(bf16)
        last = swap(forward, 2)
        parts = [(last, 0), (arrived[q], BLOCK), (kept[q], BLOCK)]
        *done, chunk = adam_chunk((master, moment, second), done, parts, q * width, tile)
        hot.append(chunk)

    from_prev = [lax.ppermute(slots[s], "dp", ahead) for s in range(COLD - 1)]
    from_next = [lax.ppermute(slots[s], "dp", back) for s in range(1, COLD)]

    hot_weights = jnp.zeros((BLOCK, n_t * qlocal), bf16)
    for q in range(CHUNKS):
        up, down = [hot[q]], [hot[q]]
        for k in range(1, n_t):
            up.append(lax.ppermute(up[-1], "tensor", [(i, i + 1) for i in range(k - 1, n_t - 1)]))
            down.append(lax.ppermute(down[-1], "tensor", [(i + 1, i) for i in range(n_t - k)]))
        hot_weights = lax.dynamic_update_slice(hot_weights, hot[q], (0, t * qlocal + q * width))
        for k in range(1, n_t):
            value = jnp.where(t >= k, up[k], down[n_t - k])
            hot_weights = lax.dynamic_update_slice(hot_weights, value, (0, (t - k) % n_t * qlocal + q * width))

    prev_dp = (dp + n_dp - 1) % n_dp
    next_dp = (dp + 1) % n_dp
    prev_flags = (ranks[prev_dp][:, None] == slot_ids[None, : COLD - 1]) & (owner_map[prev_dp] == 1)[:, None]
    next_flags = (ranks[next_dp][:, None] == slot_ids[None, 1:]) & (owner_map[next_dp] == 0)[:, None]
    flags = jnp.concatenate([prev_flags, next_flags], axis=1).astype(jnp.int32)
    cold_recv = combine_cold(flags, from_prev, from_next, tile)
    return (done[0], done[1], done[2], hot_weights, cold_recv)


def plain_device(activations, out_grad, block_ids, owner_map, master, moment, second):
    n_dp = lax.axis_size("dp")
    dp = lax.axis_index("dp")
    qlocal = out_grad.shape[1]
    rows = activations.shape[0]
    shaped = activations.reshape(rows, activations.shape[1] // BLOCK, BLOCK)
    outgoing = jax.vmap(lambda ids: shaped[:, ids, :].reshape(rows, ids.shape[0] * BLOCK))(block_ids)
    received = lax.all_to_all(outgoing, "tensor", split_axis=0, concat_axis=0, tiled=True)
    chosen = received.reshape(received.shape[0] * received.shape[1], received.shape[2])
    whole = lax.dot_general(chosen, out_grad, CONTRACT, preferred_element_type=f32).astype(bf16)
    grad = lax.psum_scatter(whole[: HOT * BLOCK], "dp", scatter_dimension=0, tiled=True).astype(f32)
    new_master, new_moment, new_second = adam(master, moment, second, grad)
    hot_weights = lax.all_gather(new_master.astype(bf16), "tensor", axis=1, tiled=True)
    cold_part = whole[HOT * BLOCK :].reshape(COLD, BLOCK, qlocal)
    from_prev = lax.ppermute(cold_part, "dp", [(i, (i + 1) % n_dp) for i in range(n_dp)])
    from_next = lax.ppermute(cold_part, "dp", [(i, (i - 1) % n_dp) for i in range(n_dp)])
    prev_owner = owner_map[(dp + n_dp - 1) % n_dp]
    next_owner = owner_map[(dp + 1) % n_dp]
    total = jnp.where((prev_owner == 1)[:, None, None], from_prev.astype(f32), 0.0)
    total = total + jnp.where((next_owner == 0)[:, None, None], from_next.astype(f32), 0.0)
    return (new_master, new_moment, new_second, hot_weights, total.reshape(COLD * BLOCK, qlocal))


def solution(mesh):
    per_device = fast_device if mesh.shape["dp"] == HOT else plain_device
    return jax.shard_map(
        per_device,
        mesh=mesh,
        in_specs=(
            P(("dp", "tensor"), None),
            P("dp", "tensor"),
            P(),
            P(),
            P("dp", "tensor"),
            P("dp", "tensor"),
            P("dp", "tensor"),
        ),
        out_specs=(
            P("dp", "tensor"),
            P("dp", "tensor"),
            P("dp", "tensor"),
            P("dp", None),
            P("dp", "tensor"),
        ),
        check_vma=False,
    )
```

```python
import jax
import jax.numpy as jnp
from jax import lax
from jax.experimental import pallas as pl
from jax.experimental.pallas import tpu as pltpu
from jax.sharding import PartitionSpec as P

BLOCK = 128
HOT = 8
COLD = 4
CHUNKS = 2

BETA_ONE = 0.9
BETA_TWO = 0.95
ADAM_EPS = 1e-08
LEARN_RATE = 0.01
DECAY = 0.1
CORRECT_ONE = 1.0 - 0.9**10
CORRECT_TWO = 1.0 - 0.95**10


f32 = jnp.float32
bf16 = jnp.bfloat16
ANY = pl.BlockSpec(memory_space=pl.ANY)
SMEM = pl.BlockSpec(memory_space=pltpu.SMEM)
VMEM = pl.BlockSpec(memory_space=pltpu.VMEM)
CONTRACT = (((0,), (0,)), ((), ()))


def adam(master, moment, second, grad):
    new_moment = BETA_ONE * moment + (1.0 - BETA_ONE) * grad
    new_second = BETA_TWO * second + (1.0 - BETA_TWO) * grad * grad
    update = new_moment / CORRECT_ONE / (jnp.sqrt(new_second / CORRECT_TWO) + ADAM_EPS)
    new_master = master - LEARN_RATE * (update + DECAY * master)
    return new_master, new_moment, new_second


def gather_blocks(activations, table, groups):
    rows = activations.shape[0]

    def body(table_ref, src, *outs):
        for out, (row, first, count) in zip(outs, groups):
            for slot in range(count):
                start = pl.multiple_of(table_ref[row, first + slot] * BLOCK, BLOCK)
                out[:, slot * BLOCK : (slot + 1) * BLOCK] = src[:, pl.ds(start, BLOCK)]

    return pl.pallas_call(
        body,
        in_specs=[SMEM, VMEM],
        out_specs=[VMEM] * len(groups),
        out_shape=[jax.ShapeDtypeStruct((rows, count * BLOCK), activations.dtype) for _, _, count in groups],
        name="gather_blocks",
    )(table, activations)


def product(place, piece_sets, rhs_list, first_col, ncols, tile, row_counts):
    nset = len(piece_sets)
    npiece = len(piece_sets[0])
    rows, width = piece_sets[0][0].shape
    depth = rows * npiece
    qlocal = rhs_list[0].shape[1]

    def body(place_ref, *rest):
        pieces = rest[: nset * npiece]
        rhs = rest[nset * npiece : nset * npiece + nset]
        outs = rest[nset * npiece + nset : -2]
        lhs, turned = rest[-2:]

        @pl.when(pl.program_id(0) == 0)
        def _():
            for s in range(nset):
                for k in range(npiece):
                    at = pl.multiple_of(s * depth + place_ref[k] * rows, rows)
                    lhs[pl.ds(at, rows), :] = pieces[s * npiece + k][...]
            turned[...] = lhs[...].T

        row = 0
        for out, count in zip(outs, row_counts):
            acc = None
            for s in range(nset):
                part = jnp.dot(
                    turned[row : row + count, s * depth : (s + 1) * depth],
                    rhs[s][...],
                    preferred_element_type=f32,
                )
                acc = part if acc is None else acc + part
            out[...] = acc.astype(out.dtype)
            row += count

    base = first_col // tile
    return pl.pallas_call(
        body,
        grid=(ncols // tile,),
        in_specs=[SMEM]
        + [pl.BlockSpec((rows, width), lambda g: (0, 0))] * (nset * npiece)
        + [pl.BlockSpec((depth, tile), lambda g: (0, base + g))] * nset,
        out_specs=[pl.BlockSpec((count, tile), lambda g: (0, g)) for count in row_counts],
        out_shape=[jax.ShapeDtypeStruct((count, ncols), bf16) for count in row_counts],
        scratch_shapes=[pltpu.VMEM((nset * depth, width), bf16), pltpu.VMEM((width, nset * depth), bf16)],
        cost_estimate=pl.CostEstimate(
            flops=2 * nset * depth * width * ncols,
            bytes_accessed=2 * (nset * depth * (width + ncols) + width * ncols),
            transcendentals=0,
        ),
        name="product",
    )(place, *[p for ps in piece_sets for p in ps], *rhs_list)


def adam_chunk(state, done, parts, first_col, tile):
    rows, qlocal = state[0].shape
    ncols = parts[0][0].shape[1]
    npart = len(parts)
    base = first_col // tile

    def body(*refs):
        ins = refs[:3]
        addends = refs[3 : 3 + npart]
        outs = refs[-4:]
        grad = addends[0][...].astype(f32)
        for ref in addends[1:]:
            grad = grad + ref[...].astype(f32)
        new = adam(ins[0][...], ins[1][...], ins[2][...], grad)
        for out, value in zip(outs[:3], new):
            out[...] = value
        outs[3][...] = new[0].astype(bf16)

    wide = pl.BlockSpec((rows, tile), lambda g: (0, base + g))
    part_specs = [pl.BlockSpec((rows, tile), lambda g, r=first // rows: (r, g)) for _, first in parts]
    extra = [] if done is None else list(done)
    return pl.pallas_call(
        body,
        grid=(ncols // tile,),
        in_specs=[wide] * 3 + part_specs + [ANY] * len(extra),
        out_specs=[wide] * 3 + [pl.BlockSpec((rows, tile), lambda g: (0, g))],
        out_shape=[jax.ShapeDtypeStruct((rows, qlocal), f32)] * 3 + [jax.ShapeDtypeStruct((rows, ncols), bf16)],
        input_output_aliases={3 + npart + i: i for i in range(len(extra))},
        cost_estimate=pl.CostEstimate(flops=20 * rows * ncols, bytes_accessed=34 * rows * ncols, transcendentals=0),
        name="adam_chunk",
    )(*state, *[p for p, _ in parts], *extra)


def combine_cold(picks, far_slots, near_slots, tile):
    slots = list(far_slots) + list(near_slots)
    rows, qlocal = slots[0].shape

    def body(picks_ref, *refs):
        out = refs[-1]
        sides = (refs[: len(far_slots)], refs[len(far_slots) : -1])
        for c in range(COLD):
            acc = None
            for side, group in enumerate(sides):
                value = jnp.zeros((rows, tile), bf16)
                for s, ref in enumerate(group):
                    value = jnp.where(picks_ref[side, c] == s, ref[...], value)
                value = value.astype(f32)
                acc = value if acc is None else acc + value
            out[c * rows : (c + 1) * rows, :] = acc

    return pl.pallas_call(
        body,
        grid=(qlocal // tile,),
        in_specs=[SMEM] + [pl.BlockSpec((rows, tile), lambda g: (0, g))] * len(slots),
        out_specs=pl.BlockSpec((COLD * rows, tile), lambda g: (0, g)),
        out_shape=jax.ShapeDtypeStruct((COLD * rows, qlocal), f32),
        cost_estimate=pl.CostEstimate(flops=48 * rows * qlocal, bytes_accessed=28 * rows * qlocal, transcendentals=0),
        name="combine_cold",
    )(picks, *slots)


def fast_device(activations, out_grad, block_ids, owner_map, master, moment, second):
    n_dp = lax.axis_size("dp")
    n_t = lax.axis_size("tensor")
    dp = lax.axis_index("dp")
    t = lax.axis_index("tensor")
    qlocal = out_grad.shape[1]
    half = n_dp // 2

    def swap(block, mask):
        return lax.ppermute(block, "dp", [(i, i ^ mask) for i in range(n_dp)])

    grad_pair = swap(out_grad, 1)

    flip = [half | 2, half, 2, 0]
    hot_order = jnp.stack([dp ^ 1 ^ m for m in flip] + [dp ^ m for m in flip])
    slot_ids = jnp.arange(COLD, dtype=jnp.int32)
    parity = (jnp.arange(n_dp, dtype=jnp.int32) % 2)[:, None]
    far = (owner_map == parity).astype(jnp.int32)
    before = (slot_ids[:, None] < slot_ids[None, :]).astype(jnp.int32)
    far_before = jnp.sum(far[:, :, None] * before[None], axis=1)
    near_before = jnp.sum((1 - far)[:, :, None] * before[None], axis=1)
    ranks = jnp.where(far == 1, far_before, jnp.sum(far, axis=1, keepdims=True) + near_before)
    my_ranks = ranks[dp]
    cold_order = jnp.sum(jnp.where(my_ranks[None, :] == slot_ids[:, None], slot_ids[None, :], 0), axis=1)
    order = jnp.concatenate([hot_order.astype(jnp.int32), HOT + cold_order.astype(jnp.int32)])
    dest = (t + jnp.arange(n_t, dtype=jnp.int32)) % n_t
    table = block_ids[dest[:, None], order[None, :]]

    pair = HOT // 2
    groups = []
    for k in range(n_t):
        groups += [(k, 0, pair), (k, pair, pair), (k, HOT, COLD)]
    gathered = gather_blocks(activations, table, groups)

    def to_group(block, k):
        if k == 0:
            return block
        return lax.ppermute(block, "tensor", [(i, (i + k) % n_t) for i in range(n_t)])

    def to_group_pair(block, k):
        route = [(d * n_t + i, (d ^ 1) * n_t + (i + k) % n_t) for d in range(n_dp) for i in range(n_t)]
        return lax.ppermute(block, ("dp", "tensor"), route)

    mine, theirs, cold = [], [], []
    for k in range(n_t):
        theirs.append(to_group_pair(gathered[3 * k], k))
        mine.append(to_group(gathered[3 * k + 1], k))
    for k in range(n_t):
        cold.append(to_group(gathered[3 * k + 2], k))
    place = (t - jnp.arange(n_t, dtype=jnp.int32)) % n_t

    width = qlocal // CHUNKS
    tile = min(512, width)
    masks = [(half, 2), (2, half)]
    kept, arrived = [], []
    for q in range(CHUNKS):
        first = masks[q % 2][0]
        counts = [BLOCK] * 4
        outs = product(place, [mine, theirs], [out_grad, grad_pair], q * width, width, tile, counts)
        flipped = 1 if first == half else 2
        kept.append((outs[3 - flipped], outs[3]))
        arrived.append((swap(outs[0], first), swap(outs[flipped], first)))

    cold, firsts = lax.optimization_barrier((cold, [pair[0] for pair in arrived]))
    slots = product(place, [cold], [out_grad], 0, qlocal, tile, [BLOCK] * COLD)

    forward = [(firsts[q].astype(f32) + kept[q][0].astype(f32)).astype(bf16) for q in range(CHUNKS)]
    last = [swap(forward[q], masks[q % 2][1]) for q in range(CHUNKS)]
    slots, last = lax.optimization_barrier((slots, last))

    done = None
    hot = []
    for q in range(CHUNKS):
        parts = [(last[q], 0), (arrived[q][1], 0), (kept[q][1], 0)]
        *done, chunk = adam_chunk((master, moment, second), done, parts, q * width, tile)
        hot.append(chunk)

    leave = [(i, (i + 1) % n_dp if i % 2 else (i - 1) % n_dp) for i in range(n_dp)]
    from_far = [lax.ppermute(slots[s], "dp", leave) for s in range(COLD - 1)]
    from_near = [swap(slots[s], 1) for s in range(1, COLD)]

    hot_weights = jnp.zeros((BLOCK, n_t * qlocal), bf16)
    ups, downs = [], []
    for q in range(CHUNKS):
        up, down = [hot[q]], [hot[q]]
        for k in range(1, n_t):
            up.append(lax.ppermute(up[-1], "tensor", [(i, i + 1) for i in range(k - 1, n_t - 1)]))
            down.append(lax.ppermute(down[-1], "tensor", [(i + 1, i) for i in range(n_t - k)]))
        ups.append(up)
        downs.append(down)

    far_dp = jnp.where(dp % 2 == 1, dp + 1, dp + n_dp - 1) % n_dp
    near_dp = dp ^ 1
    far_pick = jnp.where(far[far_dp] == 1, ranks[far_dp], -1)
    near_pick = jnp.where(far[near_dp] == 0, ranks[near_dp] - 1, -1)
    picks = jnp.stack([far_pick, near_pick]).astype(jnp.int32)
    ready = [side[q][max(n_t - 2, 0)] for side in (ups, downs) for q in range(CHUNKS)]
    from_far, from_near, ready = lax.optimization_barrier((from_far, from_near, ready))
    cold_recv = combine_cold(picks, from_far, from_near, tile)

    for q in range(CHUNKS):
        hot_weights = lax.dynamic_update_slice(hot_weights, hot[q], (0, t * qlocal + q * width))
        for k in range(1, n_t):
            value = jnp.where(t >= k, ups[q][k], downs[q][n_t - k])
            hot_weights = lax.dynamic_update_slice(hot_weights, value, (0, (t - k) % n_t * qlocal + q * width))
    return (done[0], done[1], done[2], hot_weights, cold_recv)


def plain_device(activations, out_grad, block_ids, owner_map, master, moment, second):
    n_dp = lax.axis_size("dp")
    dp = lax.axis_index("dp")
    qlocal = out_grad.shape[1]
    rows = activations.shape[0]
    shaped = activations.reshape(rows, activations.shape[1] // BLOCK, BLOCK)
    outgoing = jax.vmap(lambda ids: shaped[:, ids, :].reshape(rows, ids.shape[0] * BLOCK))(block_ids)
    received = lax.all_to_all(outgoing, "tensor", split_axis=0, concat_axis=0, tiled=True)
    chosen = received.reshape(received.shape[0] * received.shape[1], received.shape[2])
    whole = lax.dot_general(chosen, out_grad, CONTRACT, preferred_element_type=f32).astype(bf16)
    grad = lax.psum_scatter(whole[: HOT * BLOCK], "dp", scatter_dimension=0, tiled=True).astype(f32)
    new_master, new_moment, new_second = adam(master, moment, second, grad)
    hot_weights = lax.all_gather(new_master.astype(bf16), "tensor", axis=1, tiled=True)
    cold_part = whole[HOT * BLOCK :].reshape(COLD, BLOCK, qlocal)
    from_prev = lax.ppermute(cold_part, "dp", [(i, (i + 1) % n_dp) for i in range(n_dp)])
    from_next = lax.ppermute(cold_part, "dp", [(i, (i - 1) % n_dp) for i in range(n_dp)])
    prev_owner = owner_map[(dp + n_dp - 1) % n_dp]
    next_owner = owner_map[(dp + 1) % n_dp]
    total = jnp.where((prev_owner == 1)[:, None, None], from_prev.astype(f32), 0.0)
    total = total + jnp.where((next_owner == 0)[:, None, None], from_next.astype(f32), 0.0)
    return (new_master, new_moment, new_second, hot_weights, total.reshape(COLD * BLOCK, qlocal))


def solution(mesh):
    per_device = fast_device if mesh.shape["dp"] == HOT else plain_device
    return jax.shard_map(
        per_device,
        mesh=mesh,
        in_specs=(
            P(("dp", "tensor"), None),
            P("dp", "tensor"),
            P(),
            P(),
            P("dp", "tensor"),
            P("dp", "tensor"),
            P("dp", "tensor"),
        ),
        out_specs=(
            P("dp", "tensor"),
            P("dp", "tensor"),
            P("dp", "tensor"),
            P("dp", None),
            P("dp", "tensor"),
        ),
        check_vma=False,
    )
```

```python
import jax
import jax.numpy as jnp
from jax import lax
from jax.experimental import pallas as pl
from jax.experimental.pallas import tpu as pltpu
from jax.sharding import PartitionSpec as P


BLOCK = 128
HOT = 8
COLD = 4
CHUNKS = 2

BETA_ONE = 0.9
BETA_TWO = 0.95
ADAM_EPS = 1e-08
LEARN_RATE = 0.01
DECAY = 0.1
CORRECT_ONE = 1.0 - 0.9**10
CORRECT_TWO = 1.0 - 0.95**10


f32 = jnp.float32
bf16 = jnp.bfloat16
ANY = pl.BlockSpec(memory_space=pl.ANY)
SMEM = pl.BlockSpec(memory_space=pltpu.SMEM)
VMEM = pl.BlockSpec(memory_space=pltpu.VMEM)
CONTRACT = (((0,), (0,)), ((), ()))


def adam(master, moment, second, grad):
    new_moment = BETA_ONE * moment + (1.0 - BETA_ONE) * grad
    new_second = BETA_TWO * second + (1.0 - BETA_TWO) * grad * grad
    update = new_moment / CORRECT_ONE / (jnp.sqrt(new_second / CORRECT_TWO) + ADAM_EPS)
    new_master = master - LEARN_RATE * (update + DECAY * master)
    return new_master, new_moment, new_second


def gather_blocks(activations, table, groups):
    rows = activations.shape[0]

    def body(table_ref, src, *outs):
        for out, (row, first, count) in zip(outs, groups):
            for slot in range(count):
                start = pl.multiple_of(table_ref[row, first + slot] * BLOCK, BLOCK)
                out[:, slot * BLOCK : (slot + 1) * BLOCK] = src[:, pl.ds(start, BLOCK)]

    return pl.pallas_call(
        body,
        in_specs=[SMEM, VMEM],
        out_specs=[VMEM] * len(groups),
        out_shape=[jax.ShapeDtypeStruct((rows, count * BLOCK), activations.dtype) for _, _, count in groups],
        name="gather_blocks",
    )(table, activations)


def product(place, piece_sets, rhs_list, first_col, ncols, tile, row_counts):
    nset = len(piece_sets)
    npiece = len(piece_sets[0])
    rows, width = piece_sets[0][0].shape
    depth = rows * npiece

    def body(place_ref, *rest):
        pieces = rest[: nset * npiece]
        rhs = rest[nset * npiece : nset * npiece + nset]
        outs = rest[nset * npiece + nset : -2]
        lhs, turned = rest[-2:]

        @pl.when(pl.program_id(0) == 0)
        def _():
            for s in range(nset):
                for k in range(npiece):
                    at = pl.multiple_of(s * depth + place_ref[k] * rows, rows)
                    lhs[pl.ds(at, rows), :] = pieces[s * npiece + k][...]
            turned[...] = lhs[...].T

        row = 0
        for out, count in zip(outs, row_counts):
            acc = None
            for s in range(nset):
                part = jnp.dot(
                    turned[row : row + count, s * depth : (s + 1) * depth],
                    rhs[s][...],
                    preferred_element_type=f32,
                )
                acc = part if acc is None else acc + part
            out[...] = acc.astype(out.dtype)
            row += count

    base = first_col // tile
    return pl.pallas_call(
        body,
        grid=(ncols // tile,),
        in_specs=[SMEM]
        + [pl.BlockSpec((rows, width), lambda g: (0, 0))] * (nset * npiece)
        + [pl.BlockSpec((depth, tile), lambda g: (0, base + g))] * nset,
        out_specs=[pl.BlockSpec((count, tile), lambda g: (0, g)) for count in row_counts],
        out_shape=[jax.ShapeDtypeStruct((count, ncols), bf16) for count in row_counts],
        scratch_shapes=[pltpu.VMEM((nset * depth, width), bf16), pltpu.VMEM((width, nset * depth), bf16)],
        cost_estimate=pl.CostEstimate(
            flops=2 * nset * depth * width * ncols,
            bytes_accessed=2 * (nset * depth * (width + ncols) + width * ncols),
            transcendentals=0,
        ),
        name="product",
    )(place, *[p for ps in piece_sets for p in ps], *rhs_list)


def adam_chunk(state, done, parts, first_col, tile):
    rows, qlocal = state[0].shape
    ncols = parts[0][0].shape[1]
    npart = len(parts)
    base = first_col // tile

    def body(*refs):
        ins = refs[:3]
        addends = refs[3 : 3 + npart]
        outs = refs[-4:]
        grad = addends[0][...].astype(f32)
        for ref in addends[1:]:
            grad = grad + ref[...].astype(f32)
        new = adam(ins[0][...], ins[1][...], ins[2][...], grad)
        for out, value in zip(outs[:3], new):
            out[...] = value
        outs[3][...] = new[0].astype(bf16)

    wide = pl.BlockSpec((rows, tile), lambda g: (0, base + g))
    part_specs = [pl.BlockSpec((rows, tile), lambda g, r=first // rows: (r, g)) for _, first in parts]
    extra = [] if done is None else list(done)
    return pl.pallas_call(
        body,
        grid=(ncols // tile,),
        in_specs=[wide] * 3 + part_specs + [ANY] * len(extra),
        out_specs=[wide] * 3 + [pl.BlockSpec((rows, tile), lambda g: (0, g))],
        out_shape=[jax.ShapeDtypeStruct((rows, qlocal), f32)] * 3 + [jax.ShapeDtypeStruct((rows, ncols), bf16)],
        input_output_aliases={3 + npart + i: i for i in range(len(extra))},
        cost_estimate=pl.CostEstimate(flops=20 * rows * ncols, bytes_accessed=34 * rows * ncols, transcendentals=0),
        name="adam_chunk",
    )(*state, *[p for p, _ in parts], *extra)


def combine_cold(picks, far_slots, near_slots, tile):
    slots = list(far_slots) + list(near_slots)
    rows, qlocal = slots[0].shape

    def body(picks_ref, *refs):
        out = refs[-1]
        sides = (refs[: len(far_slots)], refs[len(far_slots) : -1])
        for c in range(COLD):
            acc = None
            for side, group in enumerate(sides):
                value = jnp.zeros((rows, tile), bf16)
                for s, ref in enumerate(group):
                    value = jnp.where(picks_ref[side, c] == s, ref[...], value)
                value = value.astype(f32)
                acc = value if acc is None else acc + value
            out[c * rows : (c + 1) * rows, :] = acc

    return pl.pallas_call(
        body,
        grid=(qlocal // tile,),
        in_specs=[SMEM] + [pl.BlockSpec((rows, tile), lambda g: (0, g))] * len(slots),
        out_specs=pl.BlockSpec((COLD * rows, tile), lambda g: (0, g)),
        out_shape=jax.ShapeDtypeStruct((COLD * rows, qlocal), f32),
        cost_estimate=pl.CostEstimate(flops=48 * rows * qlocal, bytes_accessed=28 * rows * qlocal, transcendentals=0),
        name="combine_cold",
    )(picks, *slots)


def fast_device(activations, out_grad, block_ids, owner_map, master, moment, second):
    n_dp = lax.axis_size("dp")
    n_t = lax.axis_size("tensor")
    dp = lax.axis_index("dp")
    t = lax.axis_index("tensor")
    qlocal = out_grad.shape[1]
    half = n_dp // 2

    def swap(block, mask):
        return lax.ppermute(block, "dp", [(i, i ^ mask) for i in range(n_dp)])

    grad_pair = swap(out_grad, 1)

    flip = [half | 2, half, 2, 0]
    hot_order = jnp.stack([dp ^ 1 ^ m for m in flip] + [dp ^ m for m in flip])
    slot_ids = jnp.arange(COLD, dtype=jnp.int32)
    parity = (jnp.arange(n_dp, dtype=jnp.int32) % 2)[:, None]
    far = (owner_map == parity).astype(jnp.int32)
    before = (slot_ids[:, None] < slot_ids[None, :]).astype(jnp.int32)
    far_before = jnp.sum(far[:, :, None] * before[None], axis=1)
    near_before = jnp.sum((1 - far)[:, :, None] * before[None], axis=1)
    ranks = jnp.where(far == 1, far_before, jnp.sum(far, axis=1, keepdims=True) + near_before)
    my_ranks = ranks[dp]
    cold_order = jnp.sum(jnp.where(my_ranks[None, :] == slot_ids[:, None], slot_ids[None, :], 0), axis=1)
    order = jnp.concatenate([hot_order.astype(jnp.int32), HOT + cold_order.astype(jnp.int32)])
    dest = (t + jnp.arange(n_t, dtype=jnp.int32)) % n_t
    table = block_ids[dest[:, None], order[None, :]]

    pair = HOT // 2
    groups = []
    for k in range(n_t):
        groups += [(k, 0, pair), (k, pair, pair), (k, HOT, COLD)]
    gathered = gather_blocks(activations, table, groups)

    def to_group(block, k):
        if k == 0:
            return block
        return lax.ppermute(block, "tensor", [(i, (i + k) % n_t) for i in range(n_t)])

    def to_group_pair(block, k):
        route = [(d * n_t + i, (d ^ 1) * n_t + (i + k) % n_t) for d in range(n_dp) for i in range(n_t)]
        return lax.ppermute(block, ("dp", "tensor"), route)

    mine, theirs, cold = [], [], []
    for k in range(n_t):
        theirs.append(to_group_pair(gathered[3 * k], k))
        mine.append(to_group(gathered[3 * k + 1], k))
    for k in range(n_t):
        cold.append(to_group(gathered[3 * k + 2], k))
    place = (t - jnp.arange(n_t, dtype=jnp.int32)) % n_t

    width = qlocal // CHUNKS
    tile = min(512, width)
    masks = [(half, 2), (2, half)]
    kept, arrived = [], []
    for q in range(CHUNKS):
        first = masks[q % 2][0]
        counts = [BLOCK] * 4
        outs = product(place, [mine, theirs], [out_grad, grad_pair], q * width, width, tile, counts)
        flipped = 1 if first == half else 2
        kept.append((outs[3 - flipped], outs[3]))
        arrived.append((swap(outs[0], first), swap(outs[flipped], first)))

    cold, firsts = lax.optimization_barrier((cold, [pair[0] for pair in arrived]))
    slots = product(place, [cold], [out_grad], 0, qlocal, tile, [BLOCK] * COLD)

    forward = [(firsts[q].astype(f32) + kept[q][0].astype(f32)).astype(bf16) for q in range(CHUNKS)]
    last = [swap(forward[q], masks[q % 2][1]) for q in range(CHUNKS)]

    done = None
    hot = []
    for q in range(CHUNKS):
        parts = [(last[q], 0), (arrived[q][1], 0), (kept[q][1], 0)]
        *done, chunk = adam_chunk((master, moment, second), done, parts, q * width, tile)
        hot.append(chunk)

    leave = [(i, (i + 1) % n_dp if i % 2 else (i - 1) % n_dp) for i in range(n_dp)]
    from_far = [lax.ppermute(slots[s], "dp", leave) for s in range(COLD - 1)]
    from_near = [swap(slots[s], 1) for s in range(1, COLD)]

    hot_weights = jnp.zeros((BLOCK, n_t * qlocal), bf16)
    ups, downs = [], []
    for q in range(CHUNKS):
        up, down = [hot[q]], [hot[q]]
        for k in range(1, n_t):
            up.append(lax.ppermute(up[-1], "tensor", [(i, i + 1) for i in range(k - 1, n_t - 1)]))
            down.append(lax.ppermute(down[-1], "tensor", [(i + 1, i) for i in range(n_t - k)]))
        ups.append(up)
        downs.append(down)

    far_dp = jnp.where(dp % 2 == 1, dp + 1, dp + n_dp - 1) % n_dp
    near_dp = dp ^ 1
    far_pick = jnp.where(far[far_dp] == 1, ranks[far_dp], -1)
    near_pick = jnp.where(far[near_dp] == 0, ranks[near_dp] - 1, -1)
    picks = jnp.stack([far_pick, near_pick]).astype(jnp.int32)
    cold_recv = combine_cold(picks, from_far, from_near, tile)

    for q in range(CHUNKS):
        hot_weights = lax.dynamic_update_slice(hot_weights, hot[q], (0, t * qlocal + q * width))
        for k in range(1, n_t):
            value = jnp.where(t >= k, ups[q][k], downs[q][n_t - k])
            hot_weights = lax.dynamic_update_slice(hot_weights, value, (0, (t - k) % n_t * qlocal + q * width))
    return (done[0], done[1], done[2], hot_weights, cold_recv)


def plain_device(activations, out_grad, block_ids, owner_map, master, moment, second):
    n_dp = lax.axis_size("dp")
    dp = lax.axis_index("dp")
    qlocal = out_grad.shape[1]
    rows = activations.shape[0]
    shaped = activations.reshape(rows, activations.shape[1] // BLOCK, BLOCK)
    outgoing = jax.vmap(lambda ids: shaped[:, ids, :].reshape(rows, ids.shape[0] * BLOCK))(block_ids)
    received = lax.all_to_all(outgoing, "tensor", split_axis=0, concat_axis=0, tiled=True)
    chosen = received.reshape(received.shape[0] * received.shape[1], received.shape[2])
    whole = lax.dot_general(chosen, out_grad, CONTRACT, preferred_element_type=f32).astype(bf16)
    grad = lax.psum_scatter(whole[: HOT * BLOCK], "dp", scatter_dimension=0, tiled=True).astype(f32)
    new_master, new_moment, new_second = adam(master, moment, second, grad)
    hot_weights = lax.all_gather(new_master.astype(bf16), "tensor", axis=1, tiled=True)
    cold_part = whole[HOT * BLOCK :].reshape(COLD, BLOCK, qlocal)
    from_prev = lax.ppermute(cold_part, "dp", [(i, (i + 1) % n_dp) for i in range(n_dp)])
    from_next = lax.ppermute(cold_part, "dp", [(i, (i - 1) % n_dp) for i in range(n_dp)])
    prev_owner = owner_map[(dp + n_dp - 1) % n_dp]
    next_owner = owner_map[(dp + 1) % n_dp]
    total = jnp.where((prev_owner == 1)[:, None, None], from_prev.astype(f32), 0.0)
    total = total + jnp.where((next_owner == 0)[:, None, None], from_next.astype(f32), 0.0)
    return (new_master, new_moment, new_second, hot_weights, total.reshape(COLD * BLOCK, qlocal))


def solution(mesh):
    fast = mesh.shape["dp"] == HOT
    per_device = fast_device if fast else plain_device
    return jax.shard_map(
        per_device,
        mesh=mesh,
        in_specs=(
            P(("dp", "tensor"), None),
            P("dp", "tensor"),
            P(),
            P(),
            P("dp", "tensor"),
            P("dp", "tensor"),
            P("dp", "tensor"),
        ),
        out_specs=(
            P("dp", "tensor"),
            P("dp", "tensor"),
            P("dp", "tensor"),
            P("dp", None),
            P("dp", "tensor"),
        ),
        check_vma=False,
    )
```
